32 devices in a mesh: row: 4 (over x, core), col: 8 (over z, y).
Axes of the slice: x: 2, y: 2, z: 4, core: 2. Of those that a mesh axis runs over, the one named last changes fastest.
Arguments:
- tiles: int32 [4, 8, 8, 128, 128], P('row', 'col'), may hold values from 0 to 1073741823, as said below
- slots: int32 [4, 8, 8], P('row', 'col'), may hold values from 0 to 31, as said below
- factor: float32 [4096, 256], P(('row', 'col')), may hold values from -0.5 to 0.5
- dual: float32 [4096, 256], P(('row', 'col')), may hold values from -0.5 to 0.5
Outputs:
- final_factor: float32 [4096, 256], P(('row', 'col'))
- final_dual: float32 [4096, 256], P(('row', 'col'))
- objective: float32 [3], replicated
- residual: float32 [3], replicated
The draws below stay inside these ranges and needn't reach their ends.
Inputs may be any that keep to these rules, and one draw needn't show every extreme that they name: `slots`: for every device, 8 distinct block numbers in ascending order. The stored blocks of all devices form a symmetric pattern: the block of rows piece p and columns piece q is stored if and only if the block of rows piece q and columns piece p is; every diagonal block is stored. `tiles`: the stored block of rows piece p and columns piece q is the transpose of the one of rows piece q and columns piece p; diagonal blocks are symmetric.
All inputs are finite; a program needn't handle non-finite values.
Results may differ from the reference program's by a relative error of at most 0.005.
Values may be sent and summed in bfloat16 or wider, within the bound.
A program may use at most 64 MiB of HBM per device.

```python
import math
import jax
import jax.numpy as jnp
from jax import lax

RANK = 256
VERT_DEV = 128
ITERS = 3
ROW_GROUPS = 4
COL_GROUPS = 8
TILES = 8
VERTICES = 4096


def piece_labels(key):
    base = jax.random.fold_in(key, 7)
    row_keys = jax.random.split(base, ROW_GROUPS)
    ranking = jax.vmap(lambda single: jax.random.permutation(single, COL_GROUPS))(row_keys)
    return (ranking * 4 // COL_GROUPS).astype(jnp.int32)


def stored_blocks(key):
    labels = piece_labels(key)
    leading = labels[:, None, :, None]
    second = labels.T[None, :, None, :]
    present = leading == second
    block_total = COL_GROUPS * ROW_GROUPS
    present = present.reshape(ROW_GROUPS, COL_GROUPS, block_total)
    places = jnp.arange(block_total, dtype=jnp.int32)
    scores = jnp.where(present, 0, block_total).astype(jnp.int32) + places
    ranking = jnp.argsort(scores, axis=-1)
    return ranking[:, :, :TILES].astype(jnp.int32)


def draw_slots(key, part):
    return stored_blocks(key)


def draw_tiles(key, part):
    chosen = stored_blocks(key)
    base = jax.random.fold_in(key, 13)
    pieces_total = ROW_GROUPS * COL_GROUPS

    def one_device(device):
        grid_row = device // COL_GROUPS
        grid_col = device % COL_GROUPS
        slots_here = chosen[grid_row, grid_col]
        row_piece = grid_row * COL_GROUPS + slots_here // ROW_GROUPS
        col_piece = slots_here % ROW_GROUPS * COL_GROUPS + grid_col

        def one_block(row_index, col_index):
            smaller = jnp.minimum(row_index, col_index)
            larger = jnp.maximum(row_index, col_index)
            block_key = jax.random.fold_in(base, smaller * pieces_total + larger)
            integers = jax.random.randint(block_key, (VERT_DEV, VERT_DEV), 0, 2 ** 30, dtype=jnp.int32)
            mirrored = jnp.triu(integers) + jnp.triu(integers, 1).T
            flipped = jnp.where(row_index > col_index, integers.T, integers)
            return jnp.where(row_index == col_index, mirrored, flipped)
        return jax.vmap(one_block)(row_piece, col_piece)
    blocks = lax.map(one_device, jnp.arange(pieces_total, dtype=jnp.int32))
    return blocks.reshape(ROW_GROUPS, COL_GROUPS, TILES, VERT_DEV, VERT_DEV)


def steps_of(key, shape, cuts, low, high):
    loudness, own = 1.0, jax.random.fold_in(key, 6)
    for dim, shards_of in cuts:
        heights = jnp.exp(jax.random.uniform(jax.random.fold_in(own, dim), (shards_of,), jnp.float32, low / len(cuts), high / len(cuts)))
        loudness = loudness * jnp.repeat(heights, shape[dim] // shards_of).reshape([-1 if axis == dim else 1 for axis in range(len(shape))])
    return loudness


def centred(key, dims, spread, reach, cuts=(), kind=jnp.bfloat16):
    values = spread * jax.random.normal(key, dims, jnp.float32)
    if cuts:
        values = values * steps_of(key, dims, cuts, -0.22, 0.18)
    return jnp.clip(values, -reach, reach).astype(kind)


def setup_inputs(seed: int = 0) -> dict:
    key_list = jax.random.split(jax.random.key(seed), 5)
    return {
        "tiles": draw_tiles(jax.random.fold_in(key_list[4], 71), 0),
        "slots": draw_slots(jax.random.fold_in(key_list[4], 71), 0),
        "factor": centred(key_list[2], (VERTICES, RANK), 0.0625, 0.5, ((0, 32),), jnp.float32),
        "dual": centred(key_list[3], (VERTICES, RANK), 0.0625, 0.5, ((0, 32),), jnp.float32),
    }


penalty = 2.0
step_size = 0.25
ridge_shift = 0.1
offset = 536870912

def block_weights(integers, vertices):
    unit_scale = math.sqrt(6.0 / vertices) / 2.0 ** 29
    return ((integers - offset).astype(jnp.float32) * unit_scale).astype(jnp.bfloat16)

def unit_rows(values):
    return values * lax.rsqrt(lax.optimization_barrier(jnp.sum(values * values, axis=1, keepdims=True)) + 1e-06)

def block_places(slots, device):
    grid_row = device // COL_GROUPS
    grid_col = device % COL_GROUPS
    stored = slots[grid_row, grid_col]
    row_piece = grid_row * COL_GROUPS + stored // ROW_GROUPS
    col_piece = stored % ROW_GROUPS * COL_GROUPS + grid_col
    return (grid_row, grid_col, row_piece, col_piece)

def reference(tiles, slots, factor, dual):
    pieces_total = ROW_GROUPS * COL_GROUPS
    devices = jnp.arange(pieces_total, dtype=jnp.int32)

    def add_rows(running, device):
        grid_row, grid_col, row_piece, col_piece = block_places(slots, device)
        weights = block_weights(tiles[grid_row, grid_col], VERTICES).astype(jnp.float32)
        return (running.at[row_piece].add(lax.optimization_barrier(jnp.sum(weights, axis=2))), None)
    initial = jnp.zeros((pieces_total, VERT_DEV), jnp.float32)
    degree = lax.scan(add_rows, initial, devices)[0].reshape(VERTICES)
    current = factor
    lagrange = dual
    projected = unit_rows(current + lagrange / penalty)
    objectives = []
    residuals = []
    for iteration in range(ITERS):
        packed = current.astype(jnp.bfloat16)
        widened = packed.astype(jnp.float32)
        pieces = widened.reshape(pieces_total, VERT_DEV, RANK)

        def add_products(running, device):
            grid_row, grid_col, row_piece, col_piece = block_places(slots, device)
            weights = block_weights(tiles[grid_row, grid_col], VERTICES).astype(jnp.float32)
            chosen = pieces[col_piece]
            products = jnp.einsum('tij,tjk->tik', weights, chosen, precision=lax.Precision.HIGHEST)
            return (running.at[row_piece].add(products), None)
        zeros_all = jnp.zeros((pieces_total, VERT_DEV, RANK), jnp.float32)
        coupled = lax.scan(add_products, zeros_all, devices)[0].reshape(VERTICES, RANK)
        gradient = degree[:, None] * widened - coupled
        gram_total = jnp.dot(packed.T.astype(jnp.float32), packed.astype(jnp.float32), preferred_element_type=jnp.float32)
        precond = RANK / VERTICES * gram_total + ridge_shift * jnp.eye(RANK, dtype=jnp.float32)
        triangle = jnp.linalg.cholesky(precond)
        descent = 2.0 * gradient - lagrange - penalty * (current - projected)
        current = current + step_size * jax.scipy.linalg.cho_solve((triangle, True), descent.T).T
        projected = unit_rows(current + lagrange / penalty)
        lagrange = lagrange + penalty * (current - projected)
        mismatch = current - projected
        objectives.append(jnp.sum(widened * gradient) / (4.0 * VERTICES))
        residuals.append(jnp.sum(mismatch * mismatch) / VERTICES)
    return (current, lagrange, jnp.stack(objectives), jnp.stack(residuals))
```

```python
import functools
import math

import jax
import jax.numpy as jnp
from jax import lax
from jax.experimental import pallas as pl
from jax.experimental.pallas import tpu as pltpu
from jax.sharding import PartitionSpec as P

ITERS = 3

penalty = 2.0
step_size = 0.25
ridge_shift = 0.1
offset = 536870912

MESH = pl.DeviceIdType.MESH
VMEM = pltpu.VMEM
HIGHEST = lax.Precision.HIGHEST
F32 = jnp.float32


def block_weights(integers, vertices):
    unit_scale = math.sqrt(6.0 / vertices) / 2.0**29
    return ((integers - offset).astype(jnp.float32) * unit_scale).astype(jnp.bfloat16)


def unit_rows(values):
    return values * lax.rsqrt(jnp.sum(values * values, axis=1, keepdims=True) + 1e-06)


def spread(dims, cols, whole, src, buf, send_sem, recv_sem, use):
    nx, nz, ny = dims
    row, col = lax.axis_index("row"), lax.axis_index("col")
    x, core = row // 2, row % 2
    if whole:
        z, y = col // ny, col % ny
    else:
        z = y = 0

    def device(xx, kk, zz, yy):
        return {"row": xx * 2 + kk, "col": zz * ny + yy if whole else col}

    def piece_of(xx, kk, zz, yy):
        return (xx * 2 + kk) * cols + zz * ny + yy

    barrier = pltpu.get_barrier_semaphore()
    mates = [device(x, core, (z + d) % nz, y) for d in range(1, nz)]
    mates += [device(x, core, z, (y + d) % ny) for d in range(1, ny)]
    mates += [device((x + d) % nx, core, z, y) for d in range(1, nx)]
    mates += [device(x, 1 - core, z, y)]
    for mate in mates:
        pl.semaphore_signal(barrier, inc=1, device_id=mate, device_id_type=MESH)
    pl.semaphore_wait(barrier, len(mates))

    def copy(ref, piece, number, mate):
        return pltpu.make_async_remote_copy(
            src_ref=ref,
            dst_ref=buf.at[piece],
            send_sem=send_sem.at[number],
            recv_sem=recv_sem.at[piece],
            device_id=mate,
            device_id_type=MESH,
        )

    me = piece_of(x, core, z, y)
    for number, mate in enumerate(mates):
        copy(src, me, number, mate).start()
    use(me, src)

    def place(m, kk):
        return piece_of((x + m // (nz * ny)) % nx, kk, (z + m % nz) % nz, (y + m // nz % ny) % ny)

    def arrive(piece):
        copy(src, piece, 0, mates[-1]).wait_recv()

    def stage(first, last, base, onward):
        def body(m, carry):
            piece = place(m, core)
            arrive(piece)
            for d, mate in enumerate(onward):
                copy(buf.at[piece], piece, base + (m - first) * len(onward) + d, mate).start()
            use(piece, buf.at[piece])
            other = place(m - 1, 1 - core)
            arrive(other)
            use(other, buf.at[other])
            return carry

        if last > first:
            lax.fori_loop(first, last, body, 0)
        return base + (last - first) * len(onward)

    base = len(mates)
    base = stage(1, nz, base, mates[nz - 1 :])
    base = stage(nz, nz * ny, base, mates[nz + ny - 2 :])
    base = stage(nz * ny, nz * ny * nx, base, mates[-1:])
    other = place(nz * ny * nx - 1, 1 - core)
    arrive(other)
    use(other, buf.at[other])

    def drain(number, carry):
        copy(src, me, number, mates[-1]).wait_send()
        return carry

    lax.fori_loop(0, base, drain, 0)


def gather_kernel(dims, cols, packed, blocks, gram, coupled, buf, send_sem, recv_sem):
    gram[...] = jnp.zeros_like(gram)
    coupled[...] = jnp.zeros_like(coupled)

    def use(piece, ref):
        value = ref[...]
        gram[...] += lax.dot_general(
            value, value, (((0,), (0,)), ((), ())), preferred_element_type=F32
        )
        coupled[...] += jnp.dot(blocks[piece], value, preferred_element_type=F32)

    spread(dims, cols, True, packed, buf, send_sem, recv_sem, use)


def tiles_kernel(dims, source, out, send_sem, recv_sem):
    def use(piece, ref):
        if ref is source:
            out[piece] = source[...]

    spread(dims, 1, False, source, out, send_sem, recv_sem, use)


def totals_kernel(dims, cols, source, out, buf, send_sem, recv_sem):
    out[...] = jnp.zeros_like(out)

    def use(piece, ref):
        out[...] += ref[...]

    spread(dims, cols, True, source, buf, send_sem, recv_sem, use)


def step_kernel(
    iteration, scale, gram, coupled, degree, current, lagrange, projected, stats,
    current_out, lagrange_out, projected_out, packed_out, stats_out, precond, inverse, rest,
):
    n = gram.shape[0]
    rows = lax.broadcasted_iota(jnp.int32, (n, n), 0)
    columns = lax.broadcasted_iota(jnp.int32, (n, n), 1)
    eye = jnp.where(rows == columns, 1.0, 0.0).astype(F32)
    matrix = scale * gram[...] + ridge_shift * eye
    precond[...] = matrix

    def exact(a, b):
        return jnp.dot(a, b, precision=HIGHEST, preferred_element_type=F32)

    def fast(a, b):
        return jnp.dot(
            a.astype(jnp.bfloat16), b.astype(jnp.bfloat16), preferred_element_type=F32
        )

    def size(value):
        return jnp.sum(value * value)

    guess = n / jnp.sum(matrix * eye)
    first = eye * guess
    remain = eye - guess * matrix
    value = first + guess * remain
    for turn in range(3):
        remain = eye - fast(precond[...], value)
        value = value + fast(value, remain)
    inverse[...] = value
    rest[...] = eye - exact(precond[...], value)
    error = size(rest[...])

    good = error < 0.25

    @pl.when(jnp.logical_not(good))
    def _():
        bound = jnp.max(jnp.sum(jnp.abs(precond[...]), axis=1, keepdims=True))
        inverse[...] = eye / bound
        rest[...] = eye - precond[...] / bound

    def unfinished(state):
        turn, left = state
        return jnp.logical_and(turn < 48, left > 1e-6)

    def turn_body(state):
        turn, left = state
        inverse[...] = inverse[...] + exact(inverse[...], rest[...])
        rest[...] = eye - exact(precond[...], inverse[...])
        return turn + 1, size(rest[...])

    lax.while_loop(unfinished, turn_body, (jnp.int32(0), jnp.where(good, error, 1e6)))

    now = current[...]
    widened = now.astype(jnp.bfloat16).astype(F32)
    gradient = degree[...] * widened - coupled[...]
    descent = 2.0 * gradient - lagrange[...] - penalty * (now - projected[...])
    solved = exact(descent, inverse[...])
    solved = solved + exact(solved, rest[...])
    now = now + step_size * solved
    current_out[...] = now
    packed_out[...] = now.astype(jnp.bfloat16)
    unit = unit_rows(now + lagrange[...] / penalty)
    projected_out[...] = unit
    mismatch = now - unit
    lagrange_out[...] = lagrange[...] + penalty * mismatch
    line = lax.broadcasted_iota(jnp.int32, stats.shape, 0)
    lane = lax.broadcasted_iota(jnp.int32, stats.shape, 1)
    here = line == iteration
    old = stats[...]
    old = jnp.where(here & (lane == 0), jnp.sum(widened * gradient), old)
    stats_out[...] = jnp.where(here & (lane == 1), jnp.sum(mismatch * mismatch), old)


def whole_specs(count):
    return [pl.BlockSpec(memory_space=VMEM)] * count


def local(tiles, slots, factor, dual):
    row_count = lax.axis_size("row")
    col_count = lax.axis_size("col")
    pieces = row_count * col_count
    piece_rows, columns = factor.shape
    vertices = piece_rows * pieces
    count = tiles.shape[2]
    ny = 2 ** (int(math.log2(col_count)) // 2)
    dims = (row_count // 2, col_count // ny, ny)
    flat = (row_count // 2, 1, 1)
    limit = 60 * 2**20

    def params(number):
        return pltpu.CompilerParams(
            collective_id=number, has_side_effects=True, vmem_limit_bytes=limit
        )

    def semaphores(number):
        return [pltpu.SemaphoreType.DMA((number,)), pltpu.SemaphoreType.DMA((number,))]

    weights = block_weights(tiles.reshape(count, piece_rows, piece_rows), vertices)
    stored = slots.reshape(1, -1).astype(jnp.bfloat16)
    stored = jnp.pad(stored, ((0, 15), (0, piece_rows - count)))
    payload = jnp.concatenate([weights.reshape(count * piece_rows, piece_rows), stored], axis=0)
    gathered = pl.pallas_call(
        functools.partial(tiles_kernel, flat),
        out_shape=jax.ShapeDtypeStruct((row_count,) + payload.shape, payload.dtype),
        in_specs=whole_specs(1),
        out_specs=pl.BlockSpec(memory_space=VMEM),
        scratch_shapes=semaphores(row_count),
        compiler_params=params(0),
    )(payload)
    mine = lax.axis_index("row")
    chosen = gathered[:, count * piece_rows, :count].astype(jnp.int32)
    wanted = jnp.arange(col_count, dtype=jnp.int32) * row_count + mine
    selector = (chosen[:, None, :] == wanted[None, :, None]).astype(jnp.bfloat16)
    source = gathered[:, : count * piece_rows].reshape(row_count, count, piece_rows, piece_rows)
    blocks = jnp.einsum("rat,rtij->raji", selector, source, preferred_element_type=jnp.bfloat16)
    blocks = blocks.reshape(pieces, piece_rows, piece_rows)
    degree = jnp.sum(blocks.astype(F32), axis=(0, 2)).reshape(piece_rows, 1)

    state = jax.ShapeDtypeStruct(factor.shape, F32)
    stats_shape = jax.ShapeDtypeStruct((8, 128), F32)
    gather = pl.pallas_call(
        functools.partial(gather_kernel, dims, col_count),
        out_shape=(jax.ShapeDtypeStruct((columns, columns), F32), state),
        in_specs=whole_specs(2),
        out_specs=tuple(whole_specs(2)),
        scratch_shapes=[VMEM((pieces, piece_rows, columns), jnp.bfloat16)] + semaphores(pieces),
        compiler_params=params(1),
    )
    current = factor
    lagrange = dual
    projected = unit_rows(current + lagrange / penalty)
    packed = factor.astype(jnp.bfloat16)
    stats = jnp.zeros((8, 128), F32)
    for iteration in range(ITERS):
        gram, coupled = gather(packed, blocks)
        current, lagrange, projected, packed, stats = pl.pallas_call(
            functools.partial(step_kernel, iteration, columns / vertices),
            out_shape=(
                state, state, state, jax.ShapeDtypeStruct(factor.shape, jnp.bfloat16), stats_shape,
            ),
            in_specs=whole_specs(7),
            out_specs=tuple(whole_specs(5)),
            scratch_shapes=[VMEM((columns, columns), F32)] * 3,
            compiler_params=pltpu.CompilerParams(vmem_limit_bytes=limit),
        )(gram, coupled, degree, current, lagrange, projected, stats)
    totals = pl.pallas_call(
        functools.partial(totals_kernel, dims, col_count),
        out_shape=stats_shape,
        in_specs=whole_specs(1),
        out_specs=pl.BlockSpec(memory_space=VMEM),
        scratch_shapes=[VMEM((pieces, 8, 128), F32)] + semaphores(pieces),
        compiler_params=params(2),
    )(stats)
    objective = totals[:ITERS, 0] / (4.0 * vertices)
    residual = totals[:ITERS, 1] / vertices
    return (current, lagrange, objective, residual)


def solution(mesh):
    in_specs = (
        P("row", "col", None, None, None),
        P("row", "col", None),
        P(("row", "col"), None),
        P(("row", "col"), None),
    )
    out_specs = (P(("row", "col"), None), P(("row", "col"), None), P(), P())
    return jax.shard_map(local, mesh=mesh, in_specs=in_specs, out_specs=out_specs, check_vma=False)
```

```python
import functools
import math

import jax
import jax.numpy as jnp
from jax import lax
from jax.experimental import pallas as pl
from jax.experimental.pallas import tpu as pltpu
from jax.sharding import PartitionSpec as P

ITERS = 3

penalty = 2.0
step_size = 0.25
ridge_shift = 0.1
offset = 536870912

MESH = pl.DeviceIdType.MESH
VMEM = pltpu.VMEM
HIGHEST = lax.Precision.HIGHEST
F32 = jnp.float32


def block_weights(integers, vertices):
    unit_scale = math.sqrt(6.0 / vertices) / 2.0**29
    return ((integers - offset).astype(jnp.float32) * unit_scale).astype(jnp.bfloat16)


def unit_rows(values):
    return values * lax.rsqrt(jnp.sum(values * values, axis=1, keepdims=True) + 1e-06)


class Place:
    def __init__(self, dims, cols, whole):
        self.nx, self.nz, self.ny = dims
        self.cols, self.whole = cols, whole
        row, self.col = lax.axis_index("row"), lax.axis_index("col")
        self.x, self.core = row // 2, row % 2
        self.z, self.y = (self.col // self.ny, self.col % self.ny) if whole else (0, 0)
        self.zs = [self.device(0, 0, d, 0) for d in range(1, self.nz)]
        self.ys = [self.device(0, 0, 0, d) for d in range(1, self.ny)]
        self.xs = [self.device(d, 0, 0, 0) for d in range(1, self.nx)]
        self.twin = self.device(0, 1, 0, 0)
        self.mates = self.zs + self.ys + self.xs + [self.twin]

    def coordinates(self, dx, dk, dz, dy):
        z, y = (self.z + dz) % self.nz, (self.y + dy) % self.ny
        return ((self.x + dx) % self.nx) * 2 + (self.core + dk) % 2, z * self.ny + y

    def device(self, dx, dk, dz, dy):
        row, col = self.coordinates(dx, dk, dz, dy)
        return {"row": row, "col": col if self.whole else self.col}

    def piece(self, dx, dk, dz, dy):
        row, col = self.coordinates(dx, dk, dz, dy)
        return row * self.cols + col

    def greet(self):
        barrier = pltpu.get_barrier_semaphore()
        for mate in self.mates:
            pl.semaphore_signal(barrier, inc=1, device_id=mate, device_id_type=MESH)
        pl.semaphore_wait(barrier, len(self.mates))


def send(src, dst, send_sem, recv_sem, mate):
    return pltpu.make_async_remote_copy(
        src_ref=src,
        dst_ref=dst,
        send_sem=send_sem,
        recv_sem=recv_sem,
        device_id=mate,
        device_id_type=MESH,
    )


def spread(dims, cols, whole, src, buf, send_sem, half_sem, recv_sem, use):
    at = Place(dims, cols, whole)
    nx, nz, ny = dims
    cut = src.shape[0] // 2
    halves = (pl.ds(0, cut), pl.ds(cut, src.shape[0] - cut))
    at.greet()

    def start(ref, piece, number, mate):
        send(ref, buf.at[piece], send_sem.at[number], recv_sem.at[0, piece], mate).start()

    def start_half(side, piece, number, mate):
        part = buf.at[piece, halves[side]]
        send(part, part, half_sem.at[side, number], recv_sem.at[side, piece], mate).start()

    def arrive(piece):
        send(src, buf.at[piece], send_sem.at[0], recv_sem.at[0, piece], at.twin).wait_recv()

    def arrive_halves(piece):
        for side in range(2):
            part = buf.at[piece, halves[side]]
            send(part, part, half_sem.at[side, 0], recv_sem.at[side, piece], at.twin).wait_recv()

    along_z = lambda j: (0, j + 1, 0)
    along_y = lambda j: (0, j % nz, 1 + j // nz)
    along_x = lambda j: (1 + j // nz, j % nz, 0)
    across = lambda j: (1 + j // (nz * (ny - 1)), j % nz, 1 + j // nz % (ny - 1))

    base = 0
    me = at.piece(0, 0, 0, 0)
    for mate in at.mates:
        start(src, me, base, mate)
        base += 1

    def piece_at(where, kk):
        dx, dz, dy = where
        return at.piece(dx, kk, dz, dy)

    def handle_z(j, base):
        piece = piece_at(along_z(j), 0)
        arrive(piece)
        onward = at.ys + at.xs + [at.twin]
        for d, mate in enumerate(onward):
            start(buf.at[piece], piece, base + j * len(onward) + d, mate)

    def handle_side(place, side, onward):
        def handle(j, base):
            piece = piece_at(place(j), 0)
            arrive(piece)
            for d, mate in enumerate(onward):
                start_half(side, piece, j * len(onward) + d, mate)
            start(buf.at[piece], piece, base + j, at.twin)

        return handle

    def handle_across(j, base):
        piece = piece_at(across(j), 0)
        arrive_halves(piece)
        start(buf.at[piece], piece, base + j, at.twin)

    count_y, count_x = nz * (ny - 1), nz * (nx - 1)
    y_item = (along_y, handle_side(along_y, 0, at.xs), 1)
    x_item = (along_x, handle_side(along_x, 1, at.ys), 1)
    groups = [(nz - 1, [(along_z, handle_z, len(at.ys) + len(at.xs) + 1)])]
    if count_y == count_x:
        groups += [(count_y, [y_item, x_item])]
    else:
        groups += [(count_y, [y_item]), (count_x, [x_item])]
    groups += [(nz * (ny - 1) * (nx - 1), [(across, handle_across, 1)])]

    def both(where, ref=None):
        twin = piece_at(where, 1)
        arrive(twin)
        piece = piece_at(where, 0)
        use(piece, twin, buf.at[piece] if ref is None else ref)

    late = [functools.partial(both, (0, 0, 0), src)]
    for count, items in groups:
        if count == 0:
            continue
        bases = []
        for _, _, sends in items:
            bases.append(base)
            base += count * sends
        for (_, handle, _), first in zip(items, bases):
            handle(0, first)
        for action in late:
            action()

        def body(j, carry, items=items, bases=bases):
            for (_, handle, _), first in zip(items, bases):
                handle(j, first)
            for place, _, _ in items:
                both(place(j - 1))
            return carry

        if count > 1:
            lax.fori_loop(1, count, body, 0)
        late = [functools.partial(both, place(count - 1)) for place, _, _ in items]
    for action in late:
        action()

    def drain(number, carry):
        send(src, buf.at[me], send_sem.at[number], recv_sem.at[0, me], at.twin).wait_send()
        return carry

    lax.fori_loop(0, base, drain, 0)
    for side, total in ((0, count_y * (nx - 1)), (1, count_x * (ny - 1))):

        def drain_half(number, carry, side=side):
            part = buf.at[me, halves[side]]
            send(part, part, half_sem.at[side, number], recv_sem.at[side, me], at.twin).wait_send()
            return carry

        if total:
            lax.fori_loop(0, total, drain_half, 0)


def gather_kernel(dims, cols, packed, blocks, gram, coupled, buf, send_sem, half_sem, recv_sem):
    gram[...] = jnp.zeros_like(gram)
    coupled[...] = jnp.zeros_like(coupled)

    def use(piece, twin, ref):
        value = jnp.concatenate([ref[...], buf[twin]], axis=0)
        weights = jnp.concatenate([blocks[piece], blocks[twin]], axis=1)
        gram[...] += lax.dot_general(
            value, value, (((0,), (0,)), ((), ())), preferred_element_type=F32
        )
        coupled[...] += jnp.dot(weights, value, preferred_element_type=F32)

    spread(dims, cols, True, packed, buf, send_sem, half_sem, recv_sem, use)


def tiles_kernel(dims, source, out, send_sem, half_sem, recv_sem):
    def use(piece, twin, ref):
        if ref is source:
            out[piece] = source[...]

    spread(dims, 1, False, source, out, send_sem, half_sem, recv_sem, use)


def totals_kernel(dims, cols, source, out, sums, buf, send_sem, recv_sem):
    at = Place(dims, cols, True)
    at.greet()
    total = source[...]
    first = 0
    copies = []
    for stage, mates in enumerate((at.zs, at.ys, at.xs, [at.twin])):
        held = source if stage == 0 else sums.at[stage]
        if stage:
            sums[stage] = total
        here = []
        for d, mate in enumerate(mates):
            slot = first + d
            here.append(send(held, buf.at[slot], send_sem.at[slot], recv_sem.at[slot], mate))
            here[-1].start()
        for d, copy in enumerate(here):
            copy.wait_recv()
            total = total + buf[first + d]
        copies += here
        first += len(mates)
    out[...] = total
    for copy in copies:
        copy.wait_send()


def step_kernel(
    iteration, scale, gram, coupled, degree, current, lagrange, projected, stats,
    current_out, lagrange_out, projected_out, packed_out, stats_out, precond, inverse, rest,
):
    n = gram.shape[0]
    rows = lax.broadcasted_iota(jnp.int32, (n, n), 0)
    columns = lax.broadcasted_iota(jnp.int32, (n, n), 1)
    eye = jnp.where(rows == columns, 1.0, 0.0).astype(F32)
    matrix = scale * gram[...] + ridge_shift * eye
    precond[...] = matrix

    def exact(a, b):
        return jnp.dot(a, b, precision=HIGHEST, preferred_element_type=F32)

    def fast(a, b):
        return jnp.dot(
            a.astype(jnp.bfloat16), b.astype(jnp.bfloat16), preferred_element_type=F32
        )

    def size(value):
        return jnp.sum(value * value)

    guess = n / jnp.sum(matrix * eye)
    first = eye * guess
    remain = eye - guess * matrix
    value = first + guess * remain
    for turn in range(3):
        remain = eye - fast(precond[...], value)
        value = value + fast(value, remain)
    inverse[...] = value
    rest[...] = eye - exact(precond[...], value)
    error = size(rest[...])

    good = error < 0.25

    @pl.when(jnp.logical_not(good))
    def _():
        bound = jnp.max(jnp.sum(jnp.abs(precond[...]), axis=1, keepdims=True))
        inverse[...] = eye / bound
        rest[...] = eye - precond[...] / bound

    def unfinished(state):
        turn, left = state
        return jnp.logical_and(turn < 48, left > 1e-6)

    def turn_body(state):
        turn, left = state
        inverse[...] = inverse[...] + exact(inverse[...], rest[...])
        rest[...] = eye - exact(precond[...], inverse[...])
        return turn + 1, size(rest[...])

    lax.while_loop(unfinished, turn_body, (jnp.int32(0), jnp.where(good, error, 1e6)))

    now = current[...]
    widened = now.astype(jnp.bfloat16).astype(F32)
    gradient = degree[...] * widened - coupled[...]
    if iteration == 0:
        before = unit_rows(now + lagrange[...] / penalty)
    else:
        before = projected[...]
    descent = 2.0 * gradient - lagrange[...] - penalty * (now - before)
    solved = exact(descent, inverse[...])
    solved = solved + exact(solved, rest[...])
    now = now + step_size * solved
    current_out[...] = now
    packed_out[...] = now.astype(jnp.bfloat16)
    unit = unit_rows(now + lagrange[...] / penalty)
    projected_out[...] = unit
    mismatch = now - unit
    lagrange_out[...] = lagrange[...] + penalty * mismatch
    line = lax.broadcasted_iota(jnp.int32, stats.shape, 0)
    lane = lax.broadcasted_iota(jnp.int32, stats.shape, 1)
    here = line == iteration
    old = jnp.zeros(stats.shape, F32) if iteration == 0 else stats[...]
    old = jnp.where(here & (lane == 0), jnp.sum(widened * gradient), old)
    stats_out[...] = jnp.where(here & (lane == 1), jnp.sum(mismatch * mismatch), old)


def whole_specs(count):
    return [pl.BlockSpec(memory_space=VMEM)] * count


def local(tiles, slots, factor, dual):
    row_count = lax.axis_size("row")
    col_count = lax.axis_size("col")
    pieces = row_count * col_count
    piece_rows, columns = factor.shape
    vertices = piece_rows * pieces
    count = tiles.shape[2]
    ny = 2 ** (int(math.log2(col_count)) // 2)
    dims = (row_count // 2, col_count // ny, ny)
    flat = (row_count // 2, 1, 1)
    limit = 60 * 2**20

    def params(number):
        return pltpu.CompilerParams(
            collective_id=number, has_side_effects=True, vmem_limit_bytes=limit
        )

    def semaphores(number):
        dma = pltpu.SemaphoreType.DMA
        return [dma((number,)), dma((2, number)), dma((2, number))]

    weights = block_weights(tiles.reshape(count, piece_rows, piece_rows), vertices)
    stored = slots.reshape(1, -1).astype(jnp.bfloat16)
    stored = jnp.pad(stored, ((0, 15), (0, piece_rows - count)))
    payload = jnp.concatenate([weights.reshape(count * piece_rows, piece_rows), stored], axis=0)
    gathered = pl.pallas_call(
        functools.partial(tiles_kernel, flat),
        out_shape=jax.ShapeDtypeStruct((row_count,) + payload.shape, payload.dtype),
        in_specs=whole_specs(1),
        out_specs=pl.BlockSpec(memory_space=VMEM),
        scratch_shapes=semaphores(row_count),
        compiler_params=params(0),
    )(payload)
    mine = lax.axis_index("row")
    chosen = gathered[:, count * piece_rows, :count].astype(jnp.int32)
    wanted = jnp.arange(col_count, dtype=jnp.int32) * row_count + mine
    selector = (chosen[:, None, :] == wanted[None, :, None]).astype(jnp.bfloat16)
    source = gathered[:, : count * piece_rows].reshape(row_count, count, piece_rows, piece_rows)
    blocks = jnp.einsum("rat,rtij->raji", selector, source, preferred_element_type=jnp.bfloat16)
    blocks = blocks.reshape(pieces, piece_rows, piece_rows)
    degree = jnp.sum(blocks.astype(F32), axis=(0, 2)).reshape(piece_rows, 1)

    state = jax.ShapeDtypeStruct(factor.shape, F32)
    stats_shape = jax.ShapeDtypeStruct((8, 128), F32)
    gather = pl.pallas_call(
        functools.partial(gather_kernel, dims, col_count),
        out_shape=(jax.ShapeDtypeStruct((columns, columns), F32), state),
        in_specs=whole_specs(2),
        out_specs=tuple(whole_specs(2)),
        scratch_shapes=[VMEM((pieces, piece_rows, columns), jnp.bfloat16)] + semaphores(pieces),
        compiler_params=params(1),
    )
    current = factor
    lagrange = dual
    projected = dual
    packed = factor.astype(jnp.bfloat16)
    stats = dual[:8, :128]
    for iteration in range(ITERS):
        gram, coupled = gather(packed, blocks)
        current, lagrange, projected, packed, stats = pl.pallas_call(
            functools.partial(step_kernel, iteration, columns / vertices),
            out_shape=(
                state, state, state, jax.ShapeDtypeStruct(factor.shape, jnp.bfloat16), stats_shape,
            ),
            in_specs=whole_specs(7),
            out_specs=tuple(whole_specs(5)),
            scratch_shapes=[VMEM((columns, columns), F32)] * 3,
            compiler_params=pltpu.CompilerParams(vmem_limit_bytes=limit),
        )(gram, coupled, degree, current, lagrange, projected, stats)
    totals = pl.pallas_call(
        functools.partial(totals_kernel, dims, col_count),
        out_shape=stats_shape,
        in_specs=whole_specs(1),
        out_specs=pl.BlockSpec(memory_space=VMEM),
        scratch_shapes=[VMEM((4, 8, 128), F32), VMEM((pieces, 8, 128), F32)]
        + [pltpu.SemaphoreType.DMA((pieces,))] * 2,
        compiler_params=params(2),
    )(stats)
    objective = totals[:ITERS, 0] / (4.0 * vertices)
    residual = totals[:ITERS, 1] / vertices
    return (current, lagrange, objective, residual)


def solution(mesh):
    in_specs = (
        P("row", "col", None, None, None),
        P("row", "col", None),
        P(("row", "col"), None),
        P(("row", "col"), None),
    )
    out_specs = (P(("row", "col"), None), P(("row", "col"), None), P(), P())
    return jax.shard_map(local, mesh=mesh, in_specs=in_specs, out_specs=out_specs, check_vma=False)
```

```python
import functools
import math

import jax
import jax.numpy as jnp
from jax import lax
from jax.experimental import pallas as pl
from jax.experimental.pallas import tpu as pltpu
from jax.sharding import PartitionSpec as P

ITERS = 3

penalty = 2.0
step_size = 0.25
ridge_shift = 0.1
offset = 536870912

MESH = pl.DeviceIdType.MESH
VMEM = pltpu.VMEM
HIGHEST = lax.Precision.HIGHEST
F32 = jnp.float32


def block_weights(integers, vertices):
    unit_scale = math.sqrt(6.0 / vertices) / 2.0**29
    return ((integers - offset).astype(jnp.float32) * unit_scale).astype(jnp.bfloat16)


def unit_rows(values):
    return values * lax.rsqrt(jnp.sum(values * values, axis=1, keepdims=True) + 1e-06)


class Place:
    def __init__(self, dims, cols, whole):
        self.nx, self.nz, self.ny = dims
        self.cols, self.whole = cols, whole
        row, self.col = lax.axis_index("row"), lax.axis_index("col")
        self.x, self.core = row // 2, row % 2
        self.z, self.y = (self.col // self.ny, self.col % self.ny) if whole else (0, 0)
        self.zs = [self.device(0, 0, d, 0) for d in range(1, self.nz)]
        self.ys = [self.device(0, 0, 0, d) for d in range(1, self.ny)]
        self.xs = [self.device(d, 0, 0, 0) for d in range(1, self.nx)]
        self.twin = self.device(0, 1, 0, 0)
        self.mates = self.zs + self.ys + self.xs + [self.twin]

    def coordinates(self, dx, dk, dz, dy):
        z, y = (self.z + dz) % self.nz, (self.y + dy) % self.ny
        return ((self.x + dx) % self.nx) * 2 + (self.core + dk) % 2, z * self.ny + y

    def device(self, dx, dk, dz, dy):
        row, col = self.coordinates(dx, dk, dz, dy)
        return {"row": row, "col": col if self.whole else self.col}

    def piece(self, dx, dk, dz, dy):
        row, col = self.coordinates(dx, dk, dz, dy)
        return row * self.cols + col

    def greet(self, mates):
        barrier = pltpu.get_barrier_semaphore()
        for mate in mates:
            pl.semaphore_signal(barrier, inc=1, device_id=mate, device_id_type=MESH)
        pl.semaphore_wait(barrier, len(mates))


def send(src, dst, send_sem, recv_sem, mate):
    return pltpu.make_async_remote_copy(
        src_ref=src,
        dst_ref=dst,
        send_sem=send_sem,
        recv_sem=recv_sem,
        device_id=mate,
        device_id_type=MESH,
    )


def spread(dims, cols, whole, src, buf, send_sem, half_sem, recv_sem, use, prelude=None):
    at = Place(dims, cols, whole)
    nx, nz, ny = dims
    cut = src.shape[0] // 2
    halves = (pl.ds(0, cut), pl.ds(cut, src.shape[0] - cut))
    at.greet(at.mates)

    def start(ref, piece, number, mate):
        send(ref, buf.at[piece], send_sem.at[number], recv_sem.at[0, piece], mate).start()

    def start_half(side, piece, number, mate):
        part = buf.at[piece, halves[side]]
        send(part, part, half_sem.at[side, number], recv_sem.at[side, piece], mate).start()

    def arrive(piece):
        send(src, buf.at[piece], send_sem.at[0], recv_sem.at[0, piece], at.twin).wait_recv()

    def arrive_halves(piece):
        for side in range(2):
            part = buf.at[piece, halves[side]]
            send(part, part, half_sem.at[side, 0], recv_sem.at[side, piece], at.twin).wait_recv()

    along_z = lambda j: (0, j + 1, 0)
    along_y = lambda j: (0, j % nz, 1 + j // nz)
    along_x = lambda j: (1 + j // nz, j % nz, 0)
    across = lambda j: (1 + j // (nz * (ny - 1)), j % nz, 1 + j // nz % (ny - 1))

    base = 0
    me = at.piece(0, 0, 0, 0)
    for mate in at.mates:
        start(src, me, base, mate)
        base += 1
    if prelude is not None:
        prelude(at)

    def piece_at(where, kk):
        dx, dz, dy = where
        return at.piece(dx, kk, dz, dy)

    def handle_z(j, base):
        piece = piece_at(along_z(j), 0)
        arrive(piece)
        onward = at.ys + at.xs + [at.twin]
        for d, mate in enumerate(onward):
            start(buf.at[piece], piece, base + j * len(onward) + d, mate)

    def handle_side(place, side, onward):
        def handle(j, base):
            piece = piece_at(place(j), 0)
            arrive(piece)
            for d, mate in enumerate(onward):
                start_half(side, piece, j * len(onward) + d, mate)
            start(buf.at[piece], piece, base + j, at.twin)

        return handle

    def handle_across(j, base):
        piece = piece_at(across(j), 0)
        arrive_halves(piece)
        start(buf.at[piece], piece, base + j, at.twin)

    count_y, count_x = nz * (ny - 1), nz * (nx - 1)
    y_item = (along_y, handle_side(along_y, 0, at.xs), 1)
    x_item = (along_x, handle_side(along_x, 1, at.ys), 1)
    groups = [(nz - 1, [(along_z, handle_z, len(at.ys) + len(at.xs) + 1)])]
    if count_y == count_x:
        groups += [(count_y, [y_item, x_item])]
    else:
        groups += [(count_y, [y_item]), (count_x, [x_item])]
    groups += [(nz * (ny - 1) * (nx - 1), [(across, handle_across, 1)])]

    def both(where, ref=None):
        twin = piece_at(where, 1)
        arrive(twin)
        piece = piece_at(where, 0)
        use(piece, twin, buf.at[piece] if ref is None else ref)

    late = [functools.partial(both, (0, 0, 0), src)]
    for count, items in groups:
        if count == 0:
            continue
        bases = []
        for _, _, sends in items:
            bases.append(base)
            base += count * sends
        for (_, handle, _), first in zip(items, bases):
            handle(0, first)
        for action in late:
            action()

        def body(j, carry, items=items, bases=bases):
            for (_, handle, _), first in zip(items, bases):
                handle(j, first)
            for place, _, _ in items:
                both(place(j - 1))
            return carry

        if count > 1:
            lax.fori_loop(1, count, body, 0)
        late = [functools.partial(both, place(count - 1)) for place, _, _ in items]
    for action in late:
        action()

    def drain(number, carry):
        send(src, buf.at[me], send_sem.at[number], recv_sem.at[0, me], at.twin).wait_send()
        return carry

    lax.fori_loop(0, base, drain, 0)
    for side, total in ((0, count_y * (nx - 1)), (1, count_x * (ny - 1))):

        def drain_half(number, carry, side=side):
            part = buf.at[me, halves[side]]
            send(part, part, half_sem.at[side, number], recv_sem.at[side, me], at.twin).wait_send()
            return carry

        if total:
            lax.fori_loop(0, total, drain_half, 0)


def gather_kernel(dims, cols, packed, blocks, gram, coupled, buf, send_sem, half_sem, recv_sem):
    gram[...] = jnp.zeros_like(gram)
    coupled[...] = jnp.zeros_like(coupled)

    def use(piece, twin, ref):
        value = jnp.concatenate([ref[...], buf[twin]], axis=0)
        weights = jnp.concatenate([blocks[piece], blocks[twin]], axis=1)
        gram[...] += lax.dot_general(
            value, value, (((0,), (0,)), ((), ())), preferred_element_type=F32
        )
        coupled[...] += jnp.dot(weights, value, preferred_element_type=F32)

    spread(dims, cols, True, packed, buf, send_sem, half_sem, recv_sem, use)


def first_kernel(
    dims, cols, vertices, tiles, places, factor, gram, gathered, shelves,
    packed, payload, send_sem, half_sem, recv_sem, tile_send, tile_recv,
):
    rows = payload.shape[0] - places.shape[0]
    packed[...] = factor[...].astype(jnp.bfloat16)
    payload[:rows] = block_weights(tiles[...], vertices)
    payload[rows:] = places[...]
    gram[...] = jnp.zeros_like(gram)
    nx = dims[0]
    chips = []

    def shelf(at, dx, dk):
        return at.coordinates(dx, dk, 0, 0)[0]

    def tile_copy(at, ref, row, number, mate):
        return send(ref, shelves.at[row], tile_send.at[number], tile_recv.at[row], mate)

    def prelude(at):
        chips.append(at)
        row = shelf(at, 0, 0)
        for number, mate in enumerate(at.xs + [at.twin]):
            tile_copy(at, payload, row, number, mate).start()
        shelves[row] = payload[...]
        gathered[at.piece(0, 0, 0, 0)] = packed[...]

    def use(piece, twin, ref):
        value = jnp.concatenate([ref[...], gathered[twin]], axis=0)
        gram[...] += lax.dot_general(
            value, value, (((0,), (0,)), ((), ())), preferred_element_type=F32
        )

    spread(dims, cols, True, packed, gathered, send_sem, half_sem, recv_sem, use, prelude)
    at = chips[0]
    for d in range(1, nx):
        row = shelf(at, d, 0)
        tile_copy(at, payload, row, 0, at.twin).wait_recv()
        tile_copy(at, shelves.at[row], row, nx - 1 + d, at.twin).start()
    for d in range(nx):
        tile_copy(at, payload, shelf(at, d, 1), 0, at.twin).wait_recv()
    for number in range(2 * nx - 1):
        tile_copy(at, payload, shelf(at, 0, 0), number, at.twin).wait_send()


def totals_kernel(dims, cols, source, out, held, buf, send_sem, recv_sem):
    at = Place(dims, cols, True)
    nx, nz, ny = dims
    far = [at.device(0, 0, i // ny, i % ny) for i in range(1, nz * ny)]
    near = [at.device(i // 2, i % 2, 0, 0) for i in range(1, 2 * nx)]
    at.greet(far + near)

    def exchange(ref, mates, first):
        copies = [
            send(ref, buf.at[first + d], send_sem.at[first + d], recv_sem.at[first + d], mate)
            for d, mate in enumerate(mates)
        ]
        for copy in copies:
            copy.start()
        total = ref[...]
        for d, copy in enumerate(copies):
            copy.wait_recv()
            total = total + buf[first + d]
        return copies, total

    sent, held[...] = exchange(source, far, 0)
    more, out[...] = exchange(held, near, len(far))
    for copy in sent + more:
        copy.wait_send()


def step_kernel(
    iteration, scale, gram, coupled, degree, current, lagrange, projected, stats,
    current_out, lagrange_out, projected_out, packed_out, stats_out, precond, inverse, rest,
):
    n = gram.shape[0]
    rows = lax.broadcasted_iota(jnp.int32, (n, n), 0)
    columns = lax.broadcasted_iota(jnp.int32, (n, n), 1)
    eye = jnp.where(rows == columns, 1.0, 0.0).astype(F32)
    matrix = scale * gram[...] + ridge_shift * eye
    precond[...] = matrix

    def exact(a, b):
        return jnp.dot(a, b, precision=HIGHEST, preferred_element_type=F32)

    def fast(a, b):
        return jnp.dot(
            a.astype(jnp.bfloat16), b.astype(jnp.bfloat16), preferred_element_type=F32
        )

    def size(value):
        return jnp.sum(value * value)

    guess = n / jnp.sum(matrix * eye)
    first = eye * guess
    remain = eye - guess * matrix
    value = first + guess * remain
    for turn in range(3):
        remain = eye - fast(precond[...], value)
        value = value + fast(value, remain)
    inverse[...] = value
    rest[...] = eye - exact(precond[...], value)
    error = size(rest[...])

    good = error < 0.25

    @pl.when(jnp.logical_not(good))
    def _():
        bound = jnp.max(jnp.sum(jnp.abs(precond[...]), axis=1, keepdims=True))
        inverse[...] = eye / bound
        rest[...] = eye - precond[...] / bound

    def unfinished(state):
        turn, left = state
        return jnp.logical_and(turn < 48, left > 1e-6)

    def turn_body(state):
        turn, left = state
        inverse[...] = inverse[...] + exact(inverse[...], rest[...])
        rest[...] = eye - exact(precond[...], inverse[...])
        return turn + 1, size(rest[...])

    lax.while_loop(unfinished, turn_body, (jnp.int32(0), jnp.where(good, error, 1e6)))

    now = current[...]
    widened = now.astype(jnp.bfloat16).astype(F32)
    gradient = degree[...] * widened - coupled[...]
    if iteration == 0:
        before = unit_rows(now + lagrange[...] / penalty)
    else:
        before = projected[...]
    descent = 2.0 * gradient - lagrange[...] - penalty * (now - before)
    solved = exact(descent, inverse[...])
    solved = solved + exact(solved, rest[...])
    now = now + step_size * solved
    current_out[...] = now
    packed_out[...] = now.astype(jnp.bfloat16)
    unit = unit_rows(now + lagrange[...] / penalty)
    projected_out[...] = unit
    mismatch = now - unit
    lagrange_out[...] = lagrange[...] + penalty * mismatch
    line = lax.broadcasted_iota(jnp.int32, stats_out.shape, 0)
    lane = lax.broadcasted_iota(jnp.int32, stats_out.shape, 1)
    here = line == iteration
    old = jnp.zeros(stats_out.shape, F32) if iteration == 0 else stats[...]
    old = jnp.where(here & (lane == 0), jnp.sum(widened * gradient), old)
    stats_out[...] = jnp.where(here & (lane == 1), jnp.sum(mismatch * mismatch), old)


def whole_specs(count):
    return [pl.BlockSpec(memory_space=VMEM)] * count


def local(tiles, slots, factor, dual):
    row_count = lax.axis_size("row")
    col_count = lax.axis_size("col")
    pieces = row_count * col_count
    piece_rows, columns = factor.shape
    vertices = piece_rows * pieces
    count = tiles.shape[2]
    ny = 2 ** (int(math.log2(col_count)) // 2)
    dims = (row_count // 2, col_count // ny, ny)
    limit = 60 * 2**20

    def params(number):
        return pltpu.CompilerParams(
            collective_id=number, has_side_effects=True, vmem_limit_bytes=limit
        )

    def semaphores(number):
        dma = pltpu.SemaphoreType.DMA
        return [dma((number,)), dma((2, number)), dma((2, number))]

    places = jnp.pad(
        slots.reshape(1, -1).astype(jnp.bfloat16), ((0, 15), (0, piece_rows - count))
    )
    gram, everything, gathered = pl.pallas_call(
        functools.partial(first_kernel, dims, col_count, vertices),
        out_shape=(
            jax.ShapeDtypeStruct((columns, columns), F32),
            jax.ShapeDtypeStruct((pieces, piece_rows, columns), jnp.bfloat16),
            jax.ShapeDtypeStruct((row_count, count * piece_rows + 16, piece_rows), jnp.bfloat16),
        ),
        in_specs=whole_specs(3),
        out_specs=tuple(whole_specs(3)),
        scratch_shapes=[
            VMEM((piece_rows, columns), jnp.bfloat16),
            VMEM((count * piece_rows + 16, piece_rows), jnp.bfloat16),
        ]
        + semaphores(pieces)
        + [pltpu.SemaphoreType.DMA((row_count,))] * 2,
        compiler_params=params(0),
    )(tiles.reshape(count * piece_rows, piece_rows), places, factor)
    mine = lax.axis_index("row")
    chosen = gathered[:, count * piece_rows, :count].astype(jnp.int32)
    wanted = jnp.arange(col_count, dtype=jnp.int32) * row_count + mine
    selector = (chosen[:, None, :] == wanted[None, :, None]).astype(jnp.bfloat16)
    source = gathered[:, : count * piece_rows].reshape(row_count, count, piece_rows, piece_rows)
    blocks = jnp.einsum("rat,rtij->raji", selector, source, preferred_element_type=jnp.bfloat16)
    blocks = blocks.reshape(pieces, piece_rows, piece_rows)
    degree = jnp.sum(blocks.astype(F32), axis=(0, 2)).reshape(piece_rows, 1)

    state = jax.ShapeDtypeStruct(factor.shape, F32)
    stats_shape = jax.ShapeDtypeStruct((8, 128), F32)
    gather = pl.pallas_call(
        functools.partial(gather_kernel, dims, col_count),
        out_shape=(jax.ShapeDtypeStruct((columns, columns), F32), state),
        in_specs=whole_specs(2),
        out_specs=tuple(whole_specs(2)),
        scratch_shapes=[VMEM((pieces, piece_rows, columns), jnp.bfloat16)] + semaphores(pieces),
        compiler_params=params(1),
    )
    current = factor
    lagrange = dual
    projected = dual
    stats = degree
    coupled = jnp.einsum("pij,pjk->ik", blocks, everything, preferred_element_type=F32)
    for iteration in range(ITERS):
        if iteration:
            gram, coupled = gather(packed, blocks)
        current, lagrange, projected, packed, stats = pl.pallas_call(
            functools.partial(step_kernel, iteration, columns / vertices),
            out_shape=(
                state, state, state, jax.ShapeDtypeStruct(factor.shape, jnp.bfloat16), stats_shape,
            ),
            in_specs=whole_specs(7),
            out_specs=tuple(whole_specs(5)),
            scratch_shapes=[VMEM((columns, columns), F32)] * 3,
            compiler_params=pltpu.CompilerParams(vmem_limit_bytes=limit),
        )(gram, coupled, degree, current, lagrange, projected, stats)
    totals = pl.pallas_call(
        functools.partial(totals_kernel, dims, col_count),
        out_shape=stats_shape,
        in_specs=whole_specs(1),
        out_specs=pl.BlockSpec(memory_space=VMEM),
        scratch_shapes=[VMEM((8, 128), F32), VMEM((pieces, 8, 128), F32)]
        + [pltpu.SemaphoreType.DMA((pieces,))] * 2,
        compiler_params=params(2),
    )(stats)
    objective = totals[:ITERS, 0] / (4.0 * vertices)
    residual = totals[:ITERS, 1] / vertices
    return (current, lagrange, objective, residual)


def solution(mesh):
    in_specs = (
        P("row", "col", None, None, None),
        P("row", "col", None),
        P(("row", "col"), None),
        P(("row", "col"), None),
    )
    out_specs = (P(("row", "col"), None), P(("row", "col"), None), P(), P())
    return jax.shard_map(local, mesh=mesh, in_specs=in_specs, out_specs=out_specs, check_vma=False)
```

```python
import functools
import math

import jax
import jax.numpy as jnp
from jax import lax
from jax.experimental import pallas as pl
from jax.experimental.pallas import tpu as pltpu
from jax.sharding import PartitionSpec as P

ITERS = 3

penalty = 2.0
step_size = 0.25
ridge_shift = 0.1
offset = 536870912

MESH = pl.DeviceIdType.MESH
VMEM = pltpu.VMEM
HIGHEST = lax.Precision.HIGHEST
F32 = jnp.float32


def block_weights(integers, vertices):
    unit_scale = math.sqrt(6.0 / vertices) / 2.0**29
    return ((integers - offset).astype(jnp.float32) * unit_scale).astype(jnp.bfloat16)


def unit_rows(values):
    return values * lax.rsqrt(jnp.sum(values * values, axis=1, keepdims=True) + 1e-06)


class Place:
    def __init__(self, dims, cols, whole):
        self.nx, self.nz, self.ny = dims
        self.cols, self.whole = cols, whole
        row, self.col = lax.axis_index("row"), lax.axis_index("col")
        self.x, self.core = row // 2, row % 2
        self.z, self.y = (self.col // self.ny, self.col % self.ny) if whole else (0, 0)
        self.zs = [self.device(0, 0, d, 0) for d in range(1, self.nz)]
        self.ys = [self.device(0, 0, 0, d) for d in range(1, self.ny)]
        self.xs = [self.device(d, 0, 0, 0) for d in range(1, self.nx)]
        self.twin = self.device(0, 1, 0, 0)
        self.mates = self.zs + self.ys + self.xs + [self.twin]

    def coordinates(self, dx, dk, dz, dy):
        z, y = (self.z + dz) % self.nz, (self.y + dy) % self.ny
        return ((self.x + dx) % self.nx) * 2 + (self.core + dk) % 2, z * self.ny + y

    def device(self, dx, dk, dz, dy):
        row, col = self.coordinates(dx, dk, dz, dy)
        return {"row": row, "col": col if self.whole else self.col}

    def piece(self, dx, dk, dz, dy):
        row, col = self.coordinates(dx, dk, dz, dy)
        return row * self.cols + col

    def greet(self, mates):
        barrier = pltpu.get_barrier_semaphore()
        for mate in mates:
            pl.semaphore_signal(barrier, inc=1, device_id=mate, device_id_type=MESH)
        pl.semaphore_wait(barrier, len(mates))


def send(src, dst, send_sem, recv_sem, mate):
    return pltpu.make_async_remote_copy(
        src_ref=src,
        dst_ref=dst,
        send_sem=send_sem,
        recv_sem=recv_sem,
        device_id=mate,
        device_id_type=MESH,
    )


def spread(dims, cols, whole, src, buf, send_sem, half_sem, recv_sem, use, prelude=None):
    at = Place(dims, cols, whole)
    nx, nz, ny = dims
    cut = src.shape[0] // 2
    halves = (pl.ds(0, cut), pl.ds(cut, src.shape[0] - cut))
    at.greet(at.mates)

    def start(ref, piece, number, mate):
        send(ref, buf.at[piece], send_sem.at[number], recv_sem.at[0, piece], mate).start()

    def start_half(side, piece, number, mate):
        part = buf.at[piece, halves[side]]
        send(part, part, half_sem.at[side, number], recv_sem.at[side, piece], mate).start()

    def arrive(piece):
        send(src, buf.at[piece], send_sem.at[0], recv_sem.at[0, piece], at.twin).wait_recv()

    def arrive_halves(piece):
        for side in range(2):
            part = buf.at[piece, halves[side]]
            send(part, part, half_sem.at[side, 0], recv_sem.at[side, piece], at.twin).wait_recv()

    along_z = lambda j: (0, j + 1, 0)
    along_y = lambda j: (0, j % nz, 1 + j // nz)
    along_x = lambda j: (1 + j // nz, j % nz, 0)
    across = lambda j: (1 + j // (nz * (ny - 1)), j % nz, 1 + j // nz % (ny - 1))

    base = 0
    me = at.piece(0, 0, 0, 0)
    for mate in at.mates:
        start(src, me, base, mate)
        base += 1
    if prelude is not None:
        prelude(at)

    def piece_at(where, kk):
        dx, dz, dy = where
        return at.piece(dx, kk, dz, dy)

    def handle_z(j, base):
        piece = piece_at(along_z(j), 0)
        arrive(piece)
        onward = at.ys + at.xs + [at.twin]
        for d, mate in enumerate(onward):
            start(buf.at[piece], piece, base + j * len(onward) + d, mate)

    def handle_side(place, side, onward):
        def handle(j, base):
            piece = piece_at(place(j), 0)
            arrive(piece)
            for d, mate in enumerate(onward):
                start_half(side, piece, j * len(onward) + d, mate)
            start(buf.at[piece], piece, base + j, at.twin)

        return handle

    def handle_across(j, base):
        piece = piece_at(across(j), 0)
        arrive_halves(piece)
        start(buf.at[piece], piece, base + j, at.twin)

    count_y, count_x = nz * (ny - 1), nz * (nx - 1)
    y_item = (along_y, handle_side(along_y, 0, at.xs), 1)
    x_item = (along_x, handle_side(along_x, 1, at.ys), 1)
    groups = [(nz - 1, [(along_z, handle_z, len(at.ys) + len(at.xs) + 1)])]
    if count_y == count_x:
        groups += [(count_y, [y_item, x_item])]
    else:
        groups += [(count_y, [y_item]), (count_x, [x_item])]
    groups += [(nz * (ny - 1) * (nx - 1), [(across, handle_across, 1)])]

    def both(where, ref=None):
        twin = piece_at(where, 1)
        arrive(twin)
        piece = piece_at(where, 0)
        use(piece, twin, buf.at[piece] if ref is None else ref)

    late = [functools.partial(both, (0, 0, 0), src)]
    for count, items in groups:
        if count == 0:
            continue
        bases = []
        for _, _, sends in items:
            bases.append(base)
            base += count * sends
        for (_, handle, _), first in zip(items, bases):
            handle(0, first)
        for action in late:
            action()

        def body(j, carry, items=items, bases=bases):
            for (_, handle, _), first in zip(items, bases):
                handle(j, first)
            for place, _, _ in items:
                both(place(j - 1))
            return carry

        if count > 1:
            lax.fori_loop(1, count, body, 0)
        late = [functools.partial(both, place(count - 1)) for place, _, _ in items]
    for action in late:
        action()

    def drain(number, carry):
        send(src, buf.at[me], send_sem.at[number], recv_sem.at[0, me], at.twin).wait_send()
        return carry

    lax.fori_loop(0, base, drain, 0)
    for side, total in ((0, count_y * (nx - 1)), (1, count_x * (ny - 1))):

        def drain_half(number, carry, side=side):
            part = buf.at[me, halves[side]]
            send(part, part, half_sem.at[side, number], recv_sem.at[side, me], at.twin).wait_send()
            return carry

        if total:
            lax.fori_loop(0, total, drain_half, 0)


def gather_kernel(dims, cols, packed, blocks, gram, coupled, buf, send_sem, half_sem, recv_sem):
    gram[...] = jnp.zeros_like(gram)
    coupled[...] = jnp.zeros_like(coupled)

    def use(piece, twin, ref):
        value = jnp.concatenate([ref[...], buf[twin]], axis=0)
        weights = jnp.concatenate([blocks[piece], blocks[twin]], axis=0)
        gram[...] += lax.dot_general(
            value, value, (((0,), (0,)), ((), ())), preferred_element_type=F32
        )
        coupled[...] += lax.dot_general(
            weights, value, (((0,), (0,)), ((), ())), preferred_element_type=F32
        )

    spread(dims, cols, True, packed, buf, send_sem, half_sem, recv_sem, use)


def first_kernel(
    dims, cols, vertices, tiles, places, factor, gram, gathered, shelves,
    packed, payload, send_sem, half_sem, recv_sem, tile_send, tile_recv,
):
    rows = payload.shape[0] - places.shape[0]
    packed[...] = factor[...].astype(jnp.bfloat16)
    payload[:rows] = block_weights(tiles[...], vertices)
    payload[rows:] = places[...]
    gram[...] = jnp.zeros_like(gram)
    nx = dims[0]
    chips = []

    def shelf(at, dx, dk):
        return at.coordinates(dx, dk, 0, 0)[0]

    def tile_copy(at, ref, row, number, mate):
        return send(ref, shelves.at[row], tile_send.at[number], tile_recv.at[row], mate)

    def prelude(at):
        chips.append(at)
        row = shelf(at, 0, 0)
        for number, mate in enumerate(at.xs + [at.twin]):
            tile_copy(at, payload, row, number, mate).start()
        shelves[row] = payload[...]
        gathered[at.piece(0, 0, 0, 0)] = packed[...]

    def use(piece, twin, ref):
        value = jnp.concatenate([ref[...], gathered[twin]], axis=0)
        gram[...] += lax.dot_general(
            value, value, (((0,), (0,)), ((), ())), preferred_element_type=F32
        )

    spread(dims, cols, True, packed, gathered, send_sem, half_sem, recv_sem, use, prelude)
    at = chips[0]
    for d in range(1, nx):
        row = shelf(at, d, 0)
        tile_copy(at, payload, row, 0, at.twin).wait_recv()
        tile_copy(at, shelves.at[row], row, nx - 1 + d, at.twin).start()
    for d in range(nx):
        tile_copy(at, payload, shelf(at, d, 1), 0, at.twin).wait_recv()
    for number in range(2 * nx - 1):
        tile_copy(at, payload, shelf(at, 0, 0), number, at.twin).wait_send()


def totals_kernel(dims, cols, source, out, held, buf, send_sem, recv_sem):
    at = Place(dims, cols, True)
    nx, nz, ny = dims
    far = [at.device(0, 0, i // ny, i % ny) for i in range(1, nz * ny)]
    near = [at.device(i // 2, i % 2, 0, 0) for i in range(1, 2 * nx)]
    at.greet(far + near)

    def exchange(ref, mates, first):
        copies = [
            send(ref, buf.at[first + d], send_sem.at[first + d], recv_sem.at[first + d], mate)
            for d, mate in enumerate(mates)
        ]
        for copy in copies:
            copy.start()
        total = ref[...]
        for d, copy in enumerate(copies):
            copy.wait_recv()
            total = total + buf[first + d]
        return copies, total

    sent, held[...] = exchange(source, far, 0)
    more, out[...] = exchange(held, near, len(far))
    for copy in sent + more:
        copy.wait_send()


def step_kernel(
    iteration, scale, gram, coupled, degree, current, lagrange, projected, stats,
    current_out, lagrange_out, projected_out, packed_out, stats_out, precond, inverse, rest,
):
    n = gram.shape[0]
    rows = lax.broadcasted_iota(jnp.int32, (n, n), 0)
    columns = lax.broadcasted_iota(jnp.int32, (n, n), 1)
    eye = jnp.where(rows == columns, 1.0, 0.0).astype(F32)
    matrix = scale * gram[...] + ridge_shift * eye
    precond[...] = matrix

    def exact(a, b):
        return jnp.dot(a, b, precision=HIGHEST, preferred_element_type=F32)

    def fast(a, b):
        return jnp.dot(
            a.astype(jnp.bfloat16), b.astype(jnp.bfloat16), preferred_element_type=F32
        )

    def size(value):
        return jnp.sum(value * value)

    guess = n / jnp.sum(matrix * eye)
    first = eye * guess
    remain = eye - guess * matrix
    value = first + guess * remain
    for turn in range(3):
        remain = eye - fast(precond[...], value)
        value = value + fast(value, remain)
    inverse[...] = value
    rest[...] = eye - exact(precond[...], value)
    error = size(rest[...])

    good = error < 0.25

    @pl.when(jnp.logical_not(good))
    def _():
        bound = jnp.max(jnp.sum(jnp.abs(precond[...]), axis=1, keepdims=True))
        inverse[...] = eye / bound
        rest[...] = eye - precond[...] / bound

    def unfinished(state):
        turn, left = state
        return jnp.logical_and(turn < 48, left > 1e-6)

    def turn_body(state):
        turn, left = state
        inverse[...] = inverse[...] + exact(inverse[...], rest[...])
        rest[...] = eye - exact(precond[...], inverse[...])
        return turn + 1, size(rest[...])

    lax.while_loop(unfinished, turn_body, (jnp.int32(0), jnp.where(good, error, 1e6)))

    now = current[...]
    widened = now.astype(jnp.bfloat16).astype(F32)
    gradient = degree[...] * widened - coupled[...]
    if iteration == 0:
        before = unit_rows(now + lagrange[...] / penalty)
    else:
        before = projected[...]
    descent = 2.0 * gradient - lagrange[...] - penalty * (now - before)
    solved = exact(descent, inverse[...])
    solved = solved + exact(solved, rest[...])
    now = now + step_size * solved
    current_out[...] = now
    packed_out[...] = now.astype(jnp.bfloat16)
    unit = unit_rows(now + lagrange[...] / penalty)
    projected_out[...] = unit
    mismatch = now - unit
    lagrange_out[...] = lagrange[...] + penalty * mismatch
    line = lax.broadcasted_iota(jnp.int32, stats_out.shape, 0)
    lane = lax.broadcasted_iota(jnp.int32, stats_out.shape, 1)
    here = line == iteration
    old = jnp.zeros(stats_out.shape, F32) if iteration == 0 else stats[...]
    old = jnp.where(here & (lane == 0), jnp.sum(widened * gradient), old)
    stats_out[...] = jnp.where(here & (lane == 1), jnp.sum(mismatch * mismatch), old)


def whole_specs(count):
    return [pl.BlockSpec(memory_space=VMEM)] * count


def local(tiles, slots, factor, dual):
    row_count = lax.axis_size("row")
    col_count = lax.axis_size("col")
    pieces = row_count * col_count
    piece_rows, columns = factor.shape
    vertices = piece_rows * pieces
    count = tiles.shape[2]
    ny = 2 ** (int(math.log2(col_count)) // 2)
    dims = (row_count // 2, col_count // ny, ny)
    limit = 60 * 2**20

    def params(number):
        return pltpu.CompilerParams(
            collective_id=number, has_side_effects=True, vmem_limit_bytes=limit
        )

    def semaphores(number):
        dma = pltpu.SemaphoreType.DMA
        return [dma((number,)), dma((2, number)), dma((2, number))]

    places = jnp.pad(
        slots.reshape(1, -1).astype(jnp.bfloat16), ((0, 15), (0, piece_rows - count))
    )
    gram, everything, gathered = pl.pallas_call(
        functools.partial(first_kernel, dims, col_count, vertices),
        out_shape=(
            jax.ShapeDtypeStruct((columns, columns), F32),
            jax.ShapeDtypeStruct((pieces, piece_rows, columns), jnp.bfloat16),
            jax.ShapeDtypeStruct((row_count, count * piece_rows + 16, piece_rows), jnp.bfloat16),
        ),
        in_specs=whole_specs(3),
        out_specs=tuple(whole_specs(3)),
        scratch_shapes=[
            VMEM((piece_rows, columns), jnp.bfloat16),
            VMEM((count * piece_rows + 16, piece_rows), jnp.bfloat16),
        ]
        + semaphores(pieces)
        + [pltpu.SemaphoreType.DMA((row_count,))] * 2,
        compiler_params=params(0),
    )(tiles.reshape(count * piece_rows, piece_rows), places, factor)
    mine = lax.axis_index("row")
    chosen = gathered[:, count * piece_rows, :count].astype(jnp.int32)
    wanted = jnp.arange(col_count, dtype=jnp.int32) * row_count + mine
    selector = (chosen[:, None, :] == wanted[None, :, None]).astype(jnp.bfloat16)
    source = gathered[:, : count * piece_rows].reshape(row_count, count, piece_rows, piece_rows)
    blocks = jnp.einsum("rat,rtij->raij", selector, source, preferred_element_type=jnp.bfloat16)
    blocks = blocks.reshape(pieces, piece_rows, piece_rows)
    degree = jnp.sum(blocks.astype(F32), axis=(0, 1)).reshape(piece_rows, 1)

    state = jax.ShapeDtypeStruct(factor.shape, F32)
    stats_shape = jax.ShapeDtypeStruct((8, 128), F32)
    gather = pl.pallas_call(
        functools.partial(gather_kernel, dims, col_count),
        out_shape=(jax.ShapeDtypeStruct((columns, columns), F32), state),
        in_specs=whole_specs(2),
        out_specs=tuple(whole_specs(2)),
        scratch_shapes=[VMEM((pieces, piece_rows, columns), jnp.bfloat16)] + semaphores(pieces),
        compiler_params=params(1),
    )
    current = factor
    lagrange = dual
    projected = dual
    stats = degree
    coupled = jnp.einsum("pji,pjk->ik", blocks, everything, preferred_element_type=F32)
    for iteration in range(ITERS):
        if iteration:
            gram, coupled = gather(packed, blocks)
        current, lagrange, projected, packed, stats = pl.pallas_call(
            functools.partial(step_kernel, iteration, columns / vertices),
            out_shape=(
                state, state, state, jax.ShapeDtypeStruct(factor.shape, jnp.bfloat16), stats_shape,
            ),
            in_specs=whole_specs(7),
            out_specs=tuple(whole_specs(5)),
            scratch_shapes=[VMEM((columns, columns), F32)] * 3,
            compiler_params=pltpu.CompilerParams(vmem_limit_bytes=limit),
        )(gram, coupled, degree, current, lagrange, projected, stats)
    totals = pl.pallas_call(
        functools.partial(totals_kernel, dims, col_count),
        out_shape=stats_shape,
        in_specs=whole_specs(1),
        out_specs=pl.BlockSpec(memory_space=VMEM),
        scratch_shapes=[VMEM((8, 128), F32), VMEM((pieces, 8, 128), F32)]
        + [pltpu.SemaphoreType.DMA((pieces,))] * 2,
        compiler_params=params(2),
    )(stats)
    objective = totals[:ITERS, 0] / (4.0 * vertices)
    residual = totals[:ITERS, 1] / vertices
    return (current, lagrange, objective, residual)


def solution(mesh):
    in_specs = (
        P("row", "col", None, None, None),
        P("row", "col", None),
        P(("row", "col"), None),
        P(("row", "col"), None),
    )
    out_specs = (P(("row", "col"), None), P(("row", "col"), None), P(), P())
    return jax.shard_map(local, mesh=mesh, in_specs=in_specs, out_specs=out_specs, check_vma=False)
```
